256 devices in a mesh: zero: 64 (over z, x, core), width: 4 (over y).
Axes of the slice: x: 4, y: 4, z: 8, core: 2. Of those that a mesh axis runs over, the one named last changes fastest.
Arguments:
- weight_up: bfloat16 [12288, 49152], P('zero', 'width'), may hold values from -0.15625 to 0.15625
- low_up: bfloat16 [12288, 64], P('zero'), may hold values from -0.0546875 to 0.0546875
- high_up: bfloat16 [64, 49152], P(None, 'width'), may hold values from -0.75 to 0.75
- norm_train: float32 [12288], P(('zero', 'width')), may hold values from 0.25 to 1.75
- norm_step: float32 [12288], P(('zero', 'width')), may hold values from -0.3 to 0.3
Outputs:
- ready_up: bfloat16 [12288, 49152], P(None, ('width', 'zero'))
- scale_up: float32 [49152], P(('width', 'zero'))
- serve_norm: bfloat16 [12288], replicated
The draws below stay inside these ranges and needn't reach their ends.
All inputs are finite; a program needn't handle non-finite values. Where the reference program divides by a largest or mean magnitude, that divisor is 1e-20 or more.
Results may differ from the reference program's by a relative error of at most 0.001.
Values may be sent and summed in bfloat16 or wider, within the bound.
A program may use at most 128 MiB of HBM per device.

```python
import jax
import jax.numpy as jnp

D_MODEL = 12288
D_INNER = 49152
RANK = 64


def with_spikes(array, key, source, target, blocks, factor):
    def block_of(axis_at):
        return (jnp.arange(array.shape[axis_at]) // (array.shape[axis_at] // blocks)).reshape((-1,) + (1,) * (array.ndim - 1 - axis_at))

    one_side = jax.random.permutation(key, blocks)[block_of(target)]
    far = (block_of(target) + blocks // 2) % blocks
    return jnp.where((block_of(source) == one_side) | (block_of(source) == far), factor * array, array)


def level_of(own_key, dims, shards, low, top_value):
    factor_of, own = 1.0, jax.random.fold_in(own_key, 6)
    for position, blocks in shards:
        draws = jnp.exp(jax.random.uniform(jax.random.fold_in(own, position), (blocks,), jnp.float32, low / len(shards), top_value / len(shards)))
        factor_of = factor_of * jnp.repeat(draws, dims[position] // blocks).reshape([-1 if axis == position else 1 for axis in range(len(dims))])
    return factor_of


def scatter_about(stream_key, shape, spread, most, shards=(), dtype=jnp.bfloat16):
    level = level_of(stream_key, shape, shards, -0.22, 0.18) if shards else 1.0
    entries = jax.random.normal(stream_key, shape, jnp.float32) * spread * level
    return jnp.minimum(jnp.maximum(entries, -most), most).astype(dtype)


def bell_draw_with(key, extent, width, reach, split, heavy, dtype=jnp.bfloat16):
    result = width * jax.random.normal(key, extent, jnp.float32)
    if split:
        result = result * level_of(key, extent, split, -0.22, 0.18)
    return jnp.clip(with_spikes(result, jax.random.fold_in(key, 3), *heavy), -reach, reach).astype(dtype)


def setup_inputs(seed: int = 0) -> dict:
    splits = jax.random.split(jax.random.key(seed), 6)
    return {
        "weight_up": bell_draw_with(splits[0], (D_MODEL, D_INNER), D_MODEL ** -0.5, 0.15625, ((0, 64), (1, 4)), (0, 1, 64, 4.0)),
        "low_up": scatter_about(splits[1], (D_MODEL, RANK), D_MODEL ** -0.5, 0.0546875, ((0, 64),)),
        "high_up": scatter_about(splits[2], (RANK, D_INNER), RANK ** -0.5, 0.75, ((1, 4),)),
        "norm_train": jnp.clip(1.0 + 0.15 * jax.random.normal(splits[3], (D_MODEL,), jnp.float32), 0.25, 1.75),
        "norm_step": jnp.clip(jax.random.uniform(splits[4], (D_MODEL,), jnp.float32, -0.3, 0.3) * level_of(splits[4], (D_MODEL,), ((0, 256),), -0.4, 0.0), -0.3, 0.3),
    }


mix_rate = 2.0


def reference(weight_up, low_up, high_up, norm_train, norm_step):
    latest_up = weight_up.astype(jnp.float32) + mix_rate * jnp.dot(low_up, high_up, preferred_element_type=jnp.float32)
    scale_up = jnp.max(jnp.abs(latest_up), axis=0)
    ready_up = (latest_up / scale_up).astype(jnp.bfloat16)
    serve_norm = (norm_train + norm_step).astype(jnp.bfloat16)
    return ready_up, scale_up, serve_norm
```

```python
import jax
import jax.numpy as jnp
from jax import lax
from jax.experimental import pallas as pl
from jax.experimental.pallas import tpu as pltpu
from jax.sharding import Mesh
from jax.sharding import PartitionSpec as P

NZ, NX, NC, NW = 8, 4, 2, 4
CHIPS = NZ * NX
MESH = pl.DeviceIdType.MESH
ZERO = ("z", "x", "c")

MIX_RATE = 2.0
STRIDE = 13
FIRST = 5


def gather_kernel(
    weight, low_t, high, train, step,
    latest, tops, norm,
    buf, low_all, norm_all, high_own, high_turned, pick, rows,
    send_sem, full_sem, part_sem, turn_sem, phase_send, phase_recv, local_sem,
):
    z, x, c, w = (lax.axis_index(name) for name in ("z", "x", "c", "w"))
    other = 1 - c
    me = z * NX + x
    depth, rank = weight.shape[0], low_t.shape[0]
    share = rank // NW

    def at(dz=0, dx=0, dw=0, core=c):
        return {
            "z": lax.rem(z + dz + NZ, NZ),
            "x": lax.rem(x + dx + NX, NX),
            "c": core,
            "w": lax.rem(w + dw + NW, NW),
        }

    def shift(k):
        o = lax.rem(k * STRIDE, CHIPS)
        return o // NX, lax.rem(o, NX)

    def remote(src, dst, send, recv, where):
        return pltpu.make_async_remote_copy(
            src_ref=src, dst_ref=dst, send_sem=send, recv_sem=recv, device_id=where, device_id_type=MESH
        )

    barrier = pltpu.get_barrier_semaphore()

    def greet(k, carry):
        dz, dx = shift(k)
        for core in range(NC):
            pl.semaphore_signal(barrier, 1, device_id=at(dz, dx, 0, core), device_id_type=MESH)
        return carry

    lax.fori_loop(1, CHIPS, greet, 0)
    pl.semaphore_signal(barrier, 1, device_id=at(core=other), device_id_type=MESH)
    for dw in range(1, NW):
        pl.semaphore_signal(barrier, 1, device_id=at(dw=dw), device_id_type=MESH)
    pl.semaphore_wait(barrier, NC * (CHIPS - 1) + 1 + NW - 1)

    mine = pl.ds(pl.multiple_of(c * depth, 64), depth)
    part = pl.ds(pl.multiple_of(w * share, 16), share)

    def z_copies():
        out = []
        for i, dz in enumerate(range(1, NZ)):
            out.append(remote(low_t.at[part, :], low_all.at[c, x, z, part, :], phase_send.at[3 * i], phase_recv.at[3 * i], at(dz=dz)))
            out.append(remote(train, norm_all.at[c, x, z, w, 0], phase_send.at[3 * i + 1], phase_recv.at[3 * i + 1], at(dz=dz)))
            out.append(remote(step, norm_all.at[c, x, z, w, 1], phase_send.at[3 * i + 2], phase_recv.at[3 * i + 2], at(dz=dz)))
        return out

    def x_copies():
        out = []
        for i, dx in enumerate(range(1, NX)):
            s = 21 + 2 * i
            here = low_all.at[c, x, :, part, :]
            out.append(remote(here, here, phase_send.at[s], phase_recv.at[s], at(dx=dx)))
            here = norm_all.at[c, x, :, w]
            out.append(remote(here, here, phase_send.at[s + 1], phase_recv.at[s + 1], at(dx=dx)))
        return out

    def y_copies():
        out = []
        for i, dw in enumerate(range(1, NW)):
            s = 27 + 2 * i
            here = low_all.at[c, :, :, part, :]
            out.append(remote(here, here, phase_send.at[s], phase_recv.at[s], at(dw=dw)))
            here = norm_all.at[c, :, :, w]
            out.append(remote(here, here, phase_send.at[s + 1], phase_recv.at[s + 1], at(dw=dw)))
        return out

    def core_copies():
        there = at(core=other)
        return [
            remote(low_all.at[c], low_all.at[c], phase_send.at[33], phase_recv.at[33], there),
            remote(norm_all.at[c], norm_all.at[c], phase_send.at[34], phase_recv.at[34], there),
        ]

    def full_copy(k):
        dz, dx = shift(k)
        there = lax.rem(z + dz, NZ) * NX + lax.rem(x + dx, NX)
        columns = pl.ds(pl.multiple_of(there * 384 + c * 128, 128), 256)
        return remote(weight.at[:, columns], buf.at[me, mine, :], send_sem.at[0], full_sem.at[k], at(dz, dx))

    def part_copy(k):
        dz, dx = shift(k)
        there = lax.rem(z + dz, NZ) * NX + lax.rem(x + dx, NX)
        columns = pl.ds(pl.multiple_of(there * 384 + other * 256, 128), 128)
        lanes = pl.ds(pl.multiple_of(other * 128, 128), 128)
        return remote(weight.at[:, columns], buf.at[me, mine, lanes], send_sem.at[1], part_sem.at[k], at(dz, dx, 0, other))

    def source(k):
        dz, dx = shift(k)
        return lax.rem(z - dz + NZ, NZ), lax.rem(x - dx + NX, NX)

    def turn_copy(k):
        sz, sx = source(k)
        from_chip = sz * NX + sx
        return remote(
            buf.at[from_chip, mine, pl.ds(pl.multiple_of(other * 128, 128), 128)],
            buf.at[from_chip, mine, pl.ds(pl.multiple_of(c * 128, 128), 128)],
            send_sem.at[2], turn_sem.at[k], at(core=other),
        )

    def send(k, carry=0):
        full_copy(k).start()
        part_copy(k).start()
        return carry

    for copy in z_copies():
        copy.start()
    own = [
        pltpu.make_async_copy(weight.at[:, pl.ds(pl.multiple_of(me * 384 + c * 128, 128), 256)], buf.at[me, mine, :], local_sem.at[0]),
        pltpu.make_async_copy(low_t.at[part, :], low_all.at[c, x, z, part, :], local_sem.at[1]),
        pltpu.make_async_copy(train, norm_all.at[c, x, z, w, 0], local_sem.at[2]),
        pltpu.make_async_copy(step, norm_all.at[c, x, z, w, 1], local_sem.at[3]),
        pltpu.make_async_copy(high.at[:, pl.ds(pl.multiple_of(me * 384, 128), 384)], high_own, local_sem.at[4]),
    ]
    for copy in own:
        copy.start()
    lax.fori_loop(1, 1 + FIRST, send, 0)
    part_copy(0).start()

    for copy in own:
        copy.wait()
    turn_copy(0).start()
    high_turned[...] = high_own[...].astype(jnp.float32).T
    column = lax.broadcasted_iota(jnp.int32, pick.shape, 1)
    row = lax.broadcasted_iota(jnp.int32, pick.shape, 0)
    pick[...] = jnp.where(column == row + c * 64, 1.0, 0.0).astype(jnp.bfloat16)
    tops[...] = jnp.zeros_like(tops)

    sent = 1 + FIRST
    before = z_copies()
    for following in (x_copies, y_copies, core_copies):
        for copy in before:
            copy.wait_recv()
        before = following()
        for copy in before:
            copy.start()
        lax.fori_loop(sent, sent + 4, send, 0)
        sent += 4
    for copy in before:
        copy.wait_recv()
    lead = sent - 1

    for core in range(NC):
        for width in range(NW):
            def piece(chip, carry):
                both = norm_all[core, lax.rem(chip, NX), chip // NX, width]
                rows[core * NW + width, pl.ds(chip, 1), :] = both[0] + both[1]
                return carry
            lax.fori_loop(0, CHIPS, piece, 0)
    size = train.shape[1]
    flat = jnp.zeros((CHIPS, 384), jnp.float32)
    for i in range(NC * NW):
        spread = (
            lax.broadcasted_iota(jnp.int32, (size, 384), 1) == lax.broadcasted_iota(jnp.int32, (size, 384), 0) + i * size
        )
        flat += jnp.dot(
            rows[i].astype(jnp.bfloat16), jnp.where(spread, 1.0, 0.0).astype(jnp.bfloat16), preferred_element_type=jnp.float32
        )
    total = jnp.zeros(norm.shape, jnp.float32)
    for t in range(3):
        spread = lax.broadcasted_iota(jnp.int32, (96, CHIPS), 0) == 3 * lax.broadcasted_iota(jnp.int32, (96, CHIPS), 1) + t
        total += jnp.dot(
            jnp.where(spread, 1.0, 0.0).astype(jnp.bfloat16),
            flat[:, t * 128 : (t + 1) * 128].astype(jnp.bfloat16),
            preferred_element_type=jnp.float32,
        )
    norm[...] = total

    def work(k):
        turn_copy(k).wait_recv()
        sz, sx = source(k)
        chip = sz * NX + sx
        factor = high_turned[pl.ds(pl.multiple_of(c * depth, 64), depth), :].astype(jnp.bfloat16)
        base = lax.dot_general(pick[...], buf[chip], (((1,), (1,)), ((), ())), preferred_element_type=jnp.float32)
        change = jnp.concatenate(
            [jnp.dot(factor, low_all[core, sx, sz], preferred_element_type=jnp.float32) for core in range(NC)], axis=1
        )
        value = base + MIX_RATE * change
        latest[:, pl.ds(pl.multiple_of(chip * 384, 128), 384)] = value
        size_of = jnp.abs(value)
        top = jnp.maximum(jnp.maximum(size_of[:, :128], size_of[:, 128:256]), size_of[:, 256:])
        tops[...] = jnp.maximum(tops[...], top)

    part_copy(0).wait_recv()

    def main(k, carry):
        full_copy(k).wait_recv()
        part_copy(k).wait_recv()
        turn_copy(k).start()

        @pl.when(k + lead < CHIPS)
        def _():
            send(k + lead)

        work(k - 1)
        return carry

    lax.fori_loop(1, CHIPS, main, 0)
    work(CHIPS - 1)

    for copies in (z_copies, x_copies, y_copies, core_copies):
        for copy in copies():
            copy.wait_send()
    for i, of in enumerate(
        (buf.at[pl.ds(0, CHIPS - 1), pl.ds(0, depth), :], buf.at[:, pl.ds(0, depth), pl.ds(0, 128)], buf.at[:, pl.ds(0, depth), pl.ds(0, 128)])
    ):
        pltpu.make_async_copy(of, of, send_sem.at[i]).wait()


def scale_kernel(latest, tops, norm, ready, scale, serve, narrow, sems):
    top = jnp.max(tops[...], axis=1, keepdims=True)
    scale[...] = jnp.max(tops[...].T, axis=0, keepdims=True)
    serve[...] = norm[...].astype(jnp.bfloat16)
    inverse = 1.0 / top
    block = 16
    copies = []
    for i in range(latest.shape[0] // block):
        at = pl.ds(i * block, block)
        narrow[at, :] = (latest[at, :] * inverse[i * block : (i + 1) * block]).astype(jnp.bfloat16)
        copy = pltpu.make_async_copy(narrow.at[at, :], ready.at[at, :], sems.at[i])
        copy.start()
        copies.append(copy)
    for copy in copies:
        copy.wait()


def shards(weight_up, low_up, high_up, norm_train, norm_step):
    depth, inner = weight_up.shape
    rank = low_up.shape[1]
    piece = norm_train.shape[0]
    anywhere = pl.BlockSpec(memory_space=pltpu.HBM)
    in_vmem = pl.BlockSpec(memory_space=pltpu.VMEM)
    latest, tops, norm = pl.pallas_call(
        gather_kernel,
        out_shape=(
            jax.ShapeDtypeStruct((depth, inner), jnp.float32),
            jax.ShapeDtypeStruct((depth, 128), jnp.float32),
            jax.ShapeDtypeStruct((96, 128), jnp.float32),
        ),
        in_specs=[anywhere] * 5,
        out_specs=(in_vmem,) * 3,
        scratch_shapes=[
            pltpu.VMEM((CHIPS, 2 * depth, 256), jnp.bfloat16),
            pltpu.VMEM((NC, NX, NZ, rank, depth), jnp.bfloat16),
            pltpu.VMEM((NC, NX, NZ, NW, 2, 1, piece), jnp.float32),
            pltpu.VMEM((rank, 384), jnp.bfloat16),
            pltpu.VMEM((384, rank), jnp.float32),
            pltpu.VMEM((depth, 256), jnp.bfloat16),
            pltpu.VMEM((NC * NW, CHIPS, piece), jnp.float32),
            pltpu.SemaphoreType.DMA((3,)),
            pltpu.SemaphoreType.DMA((CHIPS,)),
            pltpu.SemaphoreType.DMA((CHIPS,)),
            pltpu.SemaphoreType.DMA((CHIPS,)),
            pltpu.SemaphoreType.DMA((35,)),
            pltpu.SemaphoreType.DMA((35,)),
            pltpu.SemaphoreType.DMA((5,)),
        ],
        compiler_params=pltpu.CompilerParams(collective_id=0, has_side_effects=True, vmem_limit_bytes=28 * 1024 * 1024),
        name="gather",
    )(weight_up, low_up.T, high_up, norm_train.reshape(1, piece), norm_step.reshape(1, piece))
    ready, scale, serve = pl.pallas_call(
        scale_kernel,
        out_shape=(
            jax.ShapeDtypeStruct((depth, inner), jnp.bfloat16),
            jax.ShapeDtypeStruct((1, depth), jnp.float32),
            jax.ShapeDtypeStruct((96, 128), jnp.bfloat16),
        ),
        in_specs=[in_vmem] * 3,
        out_specs=(anywhere, in_vmem, in_vmem),
        scratch_shapes=[pltpu.VMEM((depth, inner), jnp.bfloat16), pltpu.SemaphoreType.DMA((depth // 16,))],
        compiler_params=pltpu.CompilerParams(vmem_limit_bytes=28 * 1024 * 1024),
        name="scale",
    )(latest, tops, norm)
    return ready.T, scale.reshape(depth), serve.reshape(96 * 128)


def solution(mesh):
    finer = Mesh(mesh.devices.reshape(NZ, NX, NC, NW), ("z", "x", "c", "w"))
    return jax.shard_map(
        shards,
        mesh=finer,
        in_specs=(P(ZERO, "w"), P(ZERO, None), P(None, "w"), P(ZERO + ("w",)), P(ZERO + ("w",))),
        out_specs=(P(None, ("w",) + ZERO), P(("w",) + ZERO), P()),
        check_vma=False,
    )
```

```python
import jax
import jax.numpy as jnp
from jax import lax
from jax.experimental import pallas as pl
from jax.experimental.pallas import tpu as pltpu
from jax.sharding import Mesh
from jax.sharding import PartitionSpec as P

NZ, NX, NC, NW = 8, 4, 2, 4
CHIPS = NZ * NX
MESH = pl.DeviceIdType.MESH
ZERO = ("z", "x", "c")

MIX_RATE = 2.0
STRIDE = 13
FIRST = 5


def gather_kernel(
    weight, low_t, high, train, step,
    latest, tops, norm,
    buf, low_all, norm_all, high_own, high_turned, pick, rows,
    send_sem, full_sem, part_sem, turn_sem, phase_send, phase_recv, local_sem,
):
    z, x, c, w = (lax.axis_index(name) for name in ("z", "x", "c", "w"))
    other = 1 - c
    me = z * NX + x
    depth, rank = weight.shape[0], low_t.shape[0]
    share = rank // NW

    def at(dz=0, dx=0, dw=0, core=c):
        return {
            "z": lax.rem(z + dz + NZ, NZ),
            "x": lax.rem(x + dx + NX, NX),
            "c": core,
            "w": lax.rem(w + dw + NW, NW),
        }

    def shift(k):
        o = lax.rem(k * STRIDE, CHIPS)
        return o // NX, lax.rem(o, NX)

    def remote(src, dst, send, recv, where):
        return pltpu.make_async_remote_copy(
            src_ref=src, dst_ref=dst, send_sem=send, recv_sem=recv, device_id=where, device_id_type=MESH
        )

    barrier = pltpu.get_barrier_semaphore()

    def greet(k, carry):
        dz, dx = shift(k)
        for core in range(NC):
            pl.semaphore_signal(barrier, 1, device_id=at(dz, dx, 0, core), device_id_type=MESH)
        return carry

    lax.fori_loop(1, CHIPS, greet, 0)
    pl.semaphore_signal(barrier, 1, device_id=at(core=other), device_id_type=MESH)
    for dw in range(1, NW):
        pl.semaphore_signal(barrier, 1, device_id=at(dw=dw), device_id_type=MESH)
    pl.semaphore_wait(barrier, NC * (CHIPS - 1) + 1 + NW - 1)

    mine = pl.ds(pl.multiple_of(c * depth, 64), depth)
    part = pl.ds(pl.multiple_of(w * share, 16), share)

    def z_copies():
        out = []
        for i, dz in enumerate(range(1, NZ)):
            out.append(remote(low_t.at[part, :], low_all.at[c, x, z, part, :], phase_send.at[3 * i], phase_recv.at[3 * i], at(dz=dz)))
            out.append(remote(train, norm_all.at[c, x, z, w, 0], phase_send.at[3 * i + 1], phase_recv.at[3 * i + 1], at(dz=dz)))
            out.append(remote(step, norm_all.at[c, x, z, w, 1], phase_send.at[3 * i + 2], phase_recv.at[3 * i + 2], at(dz=dz)))
        return out

    def x_copies():
        out = []
        for i, dx in enumerate(range(1, NX)):
            s = 21 + 2 * i
            here = low_all.at[c, x, :, part, :]
            out.append(remote(here, here, phase_send.at[s], phase_recv.at[s], at(dx=dx)))
            here = norm_all.at[c, x, :, w]
            out.append(remote(here, here, phase_send.at[s + 1], phase_recv.at[s + 1], at(dx=dx)))
        return out

    def y_copies():
        out = []
        for i, dw in enumerate(range(1, NW)):
            s = 27 + 2 * i
            here = low_all.at[c, :, :, part, :]
            out.append(remote(here, here, phase_send.at[s], phase_recv.at[s], at(dw=dw)))
            here = norm_all.at[c, :, :, w]
            out.append(remote(here, here, phase_send.at[s + 1], phase_recv.at[s + 1], at(dw=dw)))
        return out

    def core_copies():
        there = at(core=other)
        return [
            remote(low_all.at[c], low_all.at[c], phase_send.at[33], phase_recv.at[33], there),
            remote(norm_all.at[c], norm_all.at[c], phase_send.at[34], phase_recv.at[34], there),
        ]

    def full_copy(k):
        dz, dx = shift(k)
        there = lax.rem(z + dz, NZ) * NX + lax.rem(x + dx, NX)
        columns = pl.ds(pl.multiple_of(there * 384 + c * 128, 128), 256)
        return remote(weight.at[:, columns], buf.at[me, mine, :], send_sem.at[0], full_sem.at[k], at(dz, dx))

    def part_copy(k):
        dz, dx = shift(k)
        there = lax.rem(z + dz, NZ) * NX + lax.rem(x + dx, NX)
        columns = pl.ds(pl.multiple_of(there * 384 + other * 256, 128), 128)
        lanes = pl.ds(pl.multiple_of(other * 128, 128), 128)
        return remote(weight.at[:, columns], buf.at[me, mine, lanes], send_sem.at[1], part_sem.at[k], at(dz, dx, 0, other))

    def source(k):
        dz, dx = shift(k)
        return lax.rem(z - dz + NZ, NZ), lax.rem(x - dx + NX, NX)

    def turn_copy(k):
        sz, sx = source(k)
        from_chip = sz * NX + sx
        return remote(
            buf.at[from_chip, mine, pl.ds(pl.multiple_of(other * 128, 128), 128)],
            buf.at[from_chip, mine, pl.ds(pl.multiple_of(c * 128, 128), 128)],
            send_sem.at[2], turn_sem.at[k], at(core=other),
        )

    def send(k, carry=0):
        full_copy(k).start()
        part_copy(k).start()
        return carry

    for copy in z_copies():
        copy.start()
    own = [
        pltpu.make_async_copy(weight.at[:, pl.ds(pl.multiple_of(me * 384 + c * 128, 128), 256)], buf.at[me, mine, :], local_sem.at[0]),
        pltpu.make_async_copy(low_t.at[part, :], low_all.at[c, x, z, part, :], local_sem.at[1]),
        pltpu.make_async_copy(train, norm_all.at[c, x, z, w, 0], local_sem.at[2]),
        pltpu.make_async_copy(step, norm_all.at[c, x, z, w, 1], local_sem.at[3]),
        pltpu.make_async_copy(high.at[:, pl.ds(pl.multiple_of(me * 384, 128), 384)], high_own, local_sem.at[4]),
    ]
    for copy in own:
        copy.start()
    lax.fori_loop(1, 1 + FIRST, send, 0)
    part_copy(0).start()

    for copy in own:
        copy.wait()
    turn_copy(0).start()
    high_turned[...] = high_own[...].astype(jnp.float32).T
    column = lax.broadcasted_iota(jnp.int32, pick.shape, 1)
    row = lax.broadcasted_iota(jnp.int32, pick.shape, 0)
    pick[...] = jnp.where(column == row + c * 64, 1.0, 0.0).astype(jnp.bfloat16)
    tops[...] = jnp.zeros_like(tops)

    sent = 1 + FIRST
    before = z_copies()
    for following in (x_copies, y_copies, core_copies):
        for copy in before:
            copy.wait_recv()
        before = following()
        for copy in before:
            copy.start()
        lax.fori_loop(sent, sent + 4, send, 0)
        sent += 4
    for copy in before:
        copy.wait_recv()
    lead = sent - 1

    for core in range(NC):
        for width in range(NW):
            def piece(chip, carry):
                both = norm_all[core, lax.rem(chip, NX), chip // NX, width]
                rows[core * NW + width, pl.ds(chip, 1), :] = both[0] + both[1]
                return carry
            lax.fori_loop(0, CHIPS, piece, 0)
    size = train.shape[1]
    flat = jnp.zeros((CHIPS, 384), jnp.float32)
    for i in range(NC * NW):
        spread = (
            lax.broadcasted_iota(jnp.int32, (size, 384), 1) == lax.broadcasted_iota(jnp.int32, (size, 384), 0) + i * size
        )
        flat += jnp.dot(
            rows[i].astype(jnp.bfloat16), jnp.where(spread, 1.0, 0.0).astype(jnp.bfloat16), preferred_element_type=jnp.float32
        )
    total = jnp.zeros(norm.shape, jnp.float32)
    for t in range(3):
        spread = lax.broadcasted_iota(jnp.int32, (96, CHIPS), 0) == 3 * lax.broadcasted_iota(jnp.int32, (96, CHIPS), 1) + t
        total += jnp.dot(
            jnp.where(spread, 1.0, 0.0).astype(jnp.bfloat16),
            flat[:, t * 128 : (t + 1) * 128].astype(jnp.bfloat16),
            preferred_element_type=jnp.float32,
        )
    norm[...] = total

    def work(k):
        turn_copy(k).wait_recv()
        sz, sx = source(k)
        chip = sz * NX + sx
        factor = high_turned[pl.ds(pl.multiple_of(c * depth, 64), depth), :].astype(jnp.bfloat16)
        base = lax.dot_general(pick[...], buf[chip], (((1,), (1,)), ((), ())), preferred_element_type=jnp.float32)
        change = jnp.concatenate(
            [jnp.dot(factor, low_all[core, sx, sz], preferred_element_type=jnp.float32) for core in range(NC)], axis=1
        )
        value = base + MIX_RATE * change
        latest[:, pl.ds(pl.multiple_of(chip * 384, 128), 384)] = value
        size_of = jnp.abs(value)
        top = jnp.maximum(jnp.maximum(size_of[:, :128], size_of[:, 128:256]), size_of[:, 256:])
        tops[...] = jnp.maximum(tops[...], top)

    part_copy(0).wait_recv()

    def main(k, carry):
        full_copy(k).wait_recv()
        part_copy(k).wait_recv()
        turn_copy(k).start()

        @pl.when(k + lead < CHIPS)
        def _():
            send(k + lead)

        work(k - 1)
        return carry

    lax.fori_loop(1, CHIPS, main, 0)
    work(CHIPS - 1)

    for copies in (z_copies, x_copies, y_copies, core_copies):
        for copy in copies():
            copy.wait_send()
    for i, of in enumerate(
        (buf.at[pl.ds(0, CHIPS - 1), pl.ds(0, depth), :], buf.at[:, pl.ds(0, depth), pl.ds(0, 128)], buf.at[:, pl.ds(0, depth), pl.ds(0, 128)])
    ):
        pltpu.make_async_copy(of, of, send_sem.at[i]).wait()


def scale_kernel(latest, tops, norm, ready, scale, serve, narrow, sems):
    top = jnp.max(tops[...], axis=1, keepdims=True)
    scale[...] = jnp.max(tops[...].T, axis=0, keepdims=True)
    serve[...] = norm[...].astype(jnp.bfloat16)
    inverse = 1.0 / top
    block = 16
    copies = []
    for i in range(latest.shape[0] // block):
        at = pl.ds(i * block, block)
        narrow[at, :] = (latest[at, :] * inverse[i * block : (i + 1) * block]).astype(jnp.bfloat16)
        copy = pltpu.make_async_copy(narrow.at[at, :], ready.at[at, :], sems.at[i])
        copy.start()
        copies.append(copy)
    for copy in copies:
        copy.wait()


def shards(weight_up, low_up, high_up, norm_train, norm_step):
    depth, inner = weight_up.shape
    rank = low_up.shape[1]
    piece = norm_train.shape[0]
    anywhere = pl.BlockSpec(memory_space=pltpu.HBM)
    in_vmem = pl.BlockSpec(memory_space=pltpu.VMEM)
    latest, tops, norm = pl.pallas_call(
        gather_kernel,
        out_shape=(
            jax.ShapeDtypeStruct((depth, inner), jnp.float32),
            jax.ShapeDtypeStruct((depth, 128), jnp.float32),
            jax.ShapeDtypeStruct((96, 128), jnp.float32),
        ),
        in_specs=[anywhere] * 5,
        out_specs=(in_vmem,) * 3,
        scratch_shapes=[
            pltpu.VMEM((CHIPS, 2 * depth, 256), jnp.bfloat16),
            pltpu.VMEM((NC, NX, NZ, rank, depth), jnp.bfloat16),
            pltpu.VMEM((NC, NX, NZ, NW, 2, 1, piece), jnp.float32),
            pltpu.VMEM((rank, 384), jnp.bfloat16),
            pltpu.VMEM((384, rank), jnp.float32),
            pltpu.VMEM((depth, 256), jnp.bfloat16),
            pltpu.VMEM((NC * NW, CHIPS, piece), jnp.float32),
            pltpu.SemaphoreType.DMA((3,)),
            pltpu.SemaphoreType.DMA((CHIPS,)),
            pltpu.SemaphoreType.DMA((CHIPS,)),
            pltpu.SemaphoreType.DMA((CHIPS,)),
            pltpu.SemaphoreType.DMA((35,)),
            pltpu.SemaphoreType.DMA((35,)),
            pltpu.SemaphoreType.DMA((5,)),
        ],
        compiler_params=pltpu.CompilerParams(collective_id=0, has_side_effects=True, vmem_limit_bytes=28 * 1024 * 1024),
        name="gather",
    )(
        *(
            pltpu.with_memory_space_constraint(operand, pltpu.HBM)
            for operand in (weight_up, low_up.T, high_up, norm_train.reshape(1, piece), norm_step.reshape(1, piece))
        )
    )
    ready, scale, serve = pl.pallas_call(
        scale_kernel,
        out_shape=(
            jax.ShapeDtypeStruct((depth, inner), jnp.bfloat16),
            jax.ShapeDtypeStruct((1, depth), jnp.float32),
            jax.ShapeDtypeStruct((96, 128), jnp.bfloat16),
        ),
        in_specs=[in_vmem] * 3,
        out_specs=(anywhere, in_vmem, in_vmem),
        scratch_shapes=[pltpu.VMEM((depth, inner), jnp.bfloat16), pltpu.SemaphoreType.DMA((depth // 16,))],
        compiler_params=pltpu.CompilerParams(vmem_limit_bytes=28 * 1024 * 1024),
        name="scale",
    )(latest, tops, norm)
    return ready.T, scale.reshape(depth), serve.reshape(96 * 128)


def solution(mesh):
    finer = Mesh(mesh.devices.reshape(NZ, NX, NC, NW), ("z", "x", "c", "w"))
    return jax.shard_map(
        shards,
        mesh=finer,
        in_specs=(P(ZERO, "w"), P(ZERO, None), P(None, "w"), P(ZERO + ("w",)), P(ZERO + ("w",))),
        out_specs=(P(None, ("w",) + ZERO), P(("w",) + ZERO), P()),
        check_vma=False,
    )
```

```python
import jax
import jax.numpy as jnp
from jax import lax
from jax.experimental import pallas as pl
from jax.experimental.pallas import tpu as pltpu
from jax.sharding import Mesh
from jax.sharding import PartitionSpec as P

NZ, NX, NC, NW = 8, 4, 2, 4
CHIPS = NZ * NX
MESH = pl.DeviceIdType.MESH
ZERO = ("z", "x", "c")

MIX_RATE = 2.0
ORDER = (0, 1, 4, 28, 3, 13, 26, 7, 20, 14, 27, 8, 21, 2, 15, 9, 22, 16, 29, 10, 23, 17, 30, 11, 24, 5, 18, 31, 12, 25, 6, 19)
FIRST = 4
MORE = (0, 0, 5, 5, 17, 0)


def gather_kernel(
    weight, low_t, high, train, step,
    latest, tops, norm,
    buf, low_all, norm_all, high_own, high_turned, pick, rows,
    send_sem, block_sem, turn_sem, phase_send, phase_recv, round_sem, local_sem,
):
    z, x, c, w = (lax.axis_index(name) for name in ("z", "x", "c", "w"))
    other = 1 - c
    me = z * NX + x
    depth, rank = weight.shape[0], low_t.shape[0]
    share = rank // NW

    def at(dz=0, dx=0, dw=0, core=c):
        return {
            "z": lax.rem(z + dz + NZ, NZ),
            "x": lax.rem(x + dx + NX, NX),
            "c": core,
            "w": lax.rem(w + dw + NW, NW),
        }

    def shift(k):
        word, place = k // 6, lax.rem(k, 6)
        packed, below = jnp.int32(0), jnp.int32(1)
        for i in range(6):
            packed = jnp.where(word == i, sum(o << 5 * n for n, o in enumerate(ORDER[6 * i : 6 * i + 6])), packed)
            below = jnp.where(place == i, 1 << 5 * i, below)
        o = lax.rem(packed // below, 32)
        return o // NX, lax.rem(o, NX)

    def remote(src, dst, send, recv, where):
        return pltpu.make_async_remote_copy(
            src_ref=src, dst_ref=dst, send_sem=send, recv_sem=recv, device_id=where, device_id_type=MESH
        )

    barrier = pltpu.get_barrier_semaphore()
    near = [(dz, dx, 0, core) for dz in (1, NZ - 1) for dx in range(NX) for core in (c, other)]
    near += [(0, dx, 0, core) for dx in range(1, NX) for core in (c, other)]
    near += [(0, 0, 0, other)] + [(0, 0, dw, c) for dw in range(1, NW)]
    for where in near:
        pl.semaphore_signal(barrier, 1, device_id=at(*where), device_id_type=MESH)
    pl.semaphore_wait(barrier, len(near))

    def tell(r):
        for dz in (1, NZ - 1):
            pl.semaphore_signal(round_sem.at[r], 1, device_id=at(dz), device_id_type=MESH)

    def hear(r):
        pl.semaphore_wait(round_sem.at[r], 2)

    mine = pl.ds(pl.multiple_of(c * depth, 64), depth)
    part = pl.ds(pl.multiple_of(w * share, 16), share)

    def pair(phase, low_from, low_to, norm_from, norm_to, where):
        return [
            remote(low_from, low_to, phase_send.at[phase, 0], phase_recv.at[phase, 0], where),
        ] + [remote(a, b, phase_send.at[phase, 1], phase_recv.at[phase, 1], where) for a, b in zip(norm_from, norm_to)]

    def z_copies(dz):
        here = norm_all.at[c, x, z, w]
        return pair(0, low_t.at[part, :], low_all.at[c, x, z, part, :], (train, step), (here.at[0], here.at[1]), at(dz))

    def x_copies():
        low, gain = low_all.at[c, x, :, part, :], norm_all.at[c, x, :, w]
        return [copy for dx in range(1, NX) for copy in pair(1, low, low, (gain,), (gain,), at(0, dx))]

    def y_copies():
        low, gain = low_all.at[c, :, :, part, :], norm_all.at[c, :, :, w]
        return [copy for dw in range(1, NW) for copy in pair(2, low, low, (gain,), (gain,), at(dw=dw))]

    def core_copies():
        return pair(3, low_all.at[c], low_all.at[c], (norm_all.at[c],), (norm_all.at[c],), at(core=other))

    bytes_of = (
        (low_all.at[0, 0, pl.ds(0, NZ - 1), part, :], norm_all.at[0, 0, pl.ds(0, NZ - 1), 0]),
        (low_all.at[0, pl.ds(0, NX - 1), :, part, :], norm_all.at[0, pl.ds(0, NX - 1), :, 0]),
        (low_all.at[0, :, :, pl.ds(0, share * (NW - 1)), :], norm_all.at[0, :, :, pl.ds(0, NW - 1)]),
        (low_all.at[0], norm_all.at[0]),
    )

    def wait_bytes(of, sem):
        pltpu.make_async_copy(of, of, sem).wait()

    def wait_phase(phase, sems):
        for kind in range(2):
            wait_bytes(bytes_of[phase][kind], sems.at[phase, kind])

    def full_copy(k):
        dz, dx = shift(k)
        there = lax.rem(z + dz, NZ) * NX + lax.rem(x + dx, NX)
        columns = pl.ds(pl.multiple_of(there * 384 + c * 128, 128), 256)
        return remote(weight.at[:, columns], buf.at[me, mine, :], send_sem.at[0], block_sem.at[k], at(dz, dx))

    def part_copy(k):
        dz, dx = shift(k)
        there = lax.rem(z + dz, NZ) * NX + lax.rem(x + dx, NX)
        columns = pl.ds(pl.multiple_of(there * 384 + other * 256, 128), 128)
        lanes = pl.ds(pl.multiple_of(other * 128, 128), 128)
        return remote(weight.at[:, columns], buf.at[me, mine, lanes], send_sem.at[1], block_sem.at[k], at(dz, dx, 0, other))

    def source(k):
        dz, dx = shift(k)
        return lax.rem(z - dz + NZ, NZ), lax.rem(x - dx + NX, NX)

    def turn_copy(k):
        sz, sx = source(k)
        from_chip = sz * NX + sx
        return remote(
            buf.at[from_chip, mine, pl.ds(pl.multiple_of(other * 128, 128), 128)],
            buf.at[from_chip, mine, pl.ds(pl.multiple_of(c * 128, 128), 128)],
            send_sem.at[1], turn_sem.at[lax.rem(k, 4)], at(core=other),
        )

    def send(k, carry=0):
        full_copy(k).start()
        part_copy(k).start()
        return carry

    own = [
        pltpu.make_async_copy(weight.at[:, pl.ds(pl.multiple_of(me * 384 + c * 128, 128), 256)], buf.at[me, mine, :], local_sem.at[0]),
        pltpu.make_async_copy(low_t.at[part, :], low_all.at[c, x, z, part, :], local_sem.at[1]),
        pltpu.make_async_copy(high.at[:, pl.ds(pl.multiple_of(me * 384, 128), 384)], high_own, local_sem.at[2]),
        pltpu.make_async_copy(train, norm_all.at[c, x, z, w, 0], local_sem.at[3]),
        pltpu.make_async_copy(step, norm_all.at[c, x, z, w, 1], local_sem.at[4]),
    ]
    sent = 1

    def send_more(count):
        nonlocal sent
        lax.fori_loop(sent, sent + count, send, 0)
        sent += count

    tell(0)
    for dz in (1, NZ - 1):
        for copy in z_copies(dz):
            copy.start()
    send_more(FIRST)
    for copy in own:
        copy.start()
    for r in range(3):
        hear(r)
        if r < 2:
            tell(r + 1)
        for dz in sorted({2 + r, NZ - 2 - r}):
            for copy in z_copies(dz):
                copy.start()
        send_more(MORE[r])
    part_copy(0).start()

    for copy in own:
        copy.wait()
    turn_copy(0).start()
    high_turned[...] = high_own[...].astype(jnp.float32).T
    column = lax.broadcasted_iota(jnp.int32, pick.shape, 1)
    row = lax.broadcasted_iota(jnp.int32, pick.shape, 0)
    pick[...] = jnp.where(column == row + c * 64, 1.0, 0.0).astype(jnp.bfloat16)
    tops[...] = jnp.zeros_like(tops)

    for phase, following in enumerate((x_copies, y_copies, core_copies)):
        wait_phase(phase, phase_recv)
        for copy in following():
            copy.start()
        send_more(MORE[3 + phase])
    wait_phase(3, phase_recv)
    lead = sent - 1

    for core in range(NC):
        for width in range(NW):
            def piece(chip, carry):
                both = norm_all[core, lax.rem(chip, NX), chip // NX, width]
                rows[core * NW + width, pl.ds(chip, 1), :] = both[0] + both[1]
                return carry
            lax.fori_loop(0, CHIPS, piece, 0)
    size = train.shape[1]
    flat = jnp.zeros((CHIPS, 384), jnp.float32)
    for i in range(NC * NW):
        spread = (
            lax.broadcasted_iota(jnp.int32, (size, 384), 1) == lax.broadcasted_iota(jnp.int32, (size, 384), 0) + i * size
        )
        flat += jnp.dot(
            rows[i].astype(jnp.bfloat16), jnp.where(spread, 1.0, 0.0).astype(jnp.bfloat16), preferred_element_type=jnp.float32
        )
    total = jnp.zeros(norm.shape, jnp.float32)
    for t in range(3):
        spread = lax.broadcasted_iota(jnp.int32, (96, CHIPS), 0) == 3 * lax.broadcasted_iota(jnp.int32, (96, CHIPS), 1) + t
        total += jnp.dot(
            jnp.where(spread, 1.0, 0.0).astype(jnp.bfloat16),
            flat[:, t * 128 : (t + 1) * 128].astype(jnp.bfloat16),
            preferred_element_type=jnp.float32,
        )
    norm[...] = total

    def work(k):
        turn_copy(k).wait_recv()
        sz, sx = source(k)
        chip = sz * NX + sx
        factor = high_turned[pl.ds(pl.multiple_of(c * depth, 64), depth), :].astype(jnp.bfloat16)
        base = lax.dot_general(pick[...], buf[chip], (((1,), (1,)), ((), ())), preferred_element_type=jnp.float32)
        change = jnp.concatenate(
            [jnp.dot(factor, low_all[core, sx, sz], preferred_element_type=jnp.float32) for core in range(NC)], axis=1
        )
        value = base + MIX_RATE * change
        latest[:, pl.ds(pl.multiple_of(chip * 384, 128), 384)] = value
        size_of = jnp.abs(value)
        top = jnp.maximum(jnp.maximum(size_of[:, :128], size_of[:, 128:256]), size_of[:, 256:])
        tops[...] = jnp.maximum(tops[...], top)

    wait_bytes(buf.at[0, pl.ds(0, depth), pl.ds(0, 128)], block_sem.at[0])

    def main(k, carry):
        wait_bytes(buf.at[0, pl.ds(0, depth * 3 // 2), :], block_sem.at[k])
        turn_copy(k).start()

        @pl.when(k + lead < CHIPS)
        def _():
            send(k + lead)

        work(k - 1)
        return carry

    lax.fori_loop(1, CHIPS, main, 0)
    work(CHIPS - 1)

    for phase in range(4):
        wait_phase(phase, phase_send)
    wait_bytes(buf.at[pl.ds(0, CHIPS - 1), pl.ds(0, depth), :], send_sem.at[0])
    wait_bytes(buf.at[:, pl.ds(0, depth), :], send_sem.at[1])


def scale_kernel(latest, tops, norm, ready, scale, serve, narrow, scale_row, serve_rows, sems):
    top = jnp.max(tops[...], axis=1, keepdims=True)
    inverse = 1.0 / top
    block = 16
    copies = []
    for i in range(latest.shape[0] // block):
        at = pl.ds(i * block, block)
        narrow[at, :] = (latest[at, :] * inverse[i * block : (i + 1) * block]).astype(jnp.bfloat16)
        copies.append(pltpu.make_async_copy(narrow.at[at, :], ready.at[at, :], sems.at[i]))
        copies[-1].start()
        if i == 0:
            scale_row[...] = jnp.max(tops[...].T, axis=0, keepdims=True)
            serve_rows[...] = norm[...].astype(jnp.bfloat16)
            copies.append(pltpu.make_async_copy(scale_row, scale, sems.at[latest.shape[0] // block]))
            copies[-1].start()
            copies.append(pltpu.make_async_copy(serve_rows, serve, sems.at[latest.shape[0] // block + 1]))
            copies[-1].start()
    for copy in copies:
        copy.wait()


def shards(weight_up, low_up, high_up, norm_train, norm_step):
    depth, inner = weight_up.shape
    rank = low_up.shape[1]
    piece = norm_train.shape[0]
    anywhere = pl.BlockSpec(memory_space=pltpu.HBM)
    in_vmem = pl.BlockSpec(memory_space=pltpu.VMEM)
    latest, tops, norm = pl.pallas_call(
        gather_kernel,
        out_shape=(
            jax.ShapeDtypeStruct((depth, inner), jnp.float32),
            jax.ShapeDtypeStruct((depth, 128), jnp.float32),
            jax.ShapeDtypeStruct((96, 128), jnp.float32),
        ),
        in_specs=[anywhere] * 5,
        out_specs=(in_vmem,) * 3,
        scratch_shapes=[
            pltpu.VMEM((CHIPS, 2 * depth, 256), jnp.bfloat16),
            pltpu.VMEM((NC, NX, NZ, rank, depth), jnp.bfloat16),
            pltpu.VMEM((NC, NX, NZ, NW, 2, 1, piece), jnp.float32),
            pltpu.VMEM((rank, 384), jnp.bfloat16),
            pltpu.VMEM((384, rank), jnp.float32),
            pltpu.VMEM((depth, 256), jnp.bfloat16),
            pltpu.VMEM((NC * NW, CHIPS, piece), jnp.float32),
            pltpu.SemaphoreType.DMA((2,)),
            pltpu.SemaphoreType.DMA((CHIPS,)),
            pltpu.SemaphoreType.DMA((4,)),
            pltpu.SemaphoreType.DMA((4, 2)),
            pltpu.SemaphoreType.DMA((4, 2)),
            pltpu.SemaphoreType.REGULAR((3,)),
            pltpu.SemaphoreType.DMA((5,)),
        ],
        compiler_params=pltpu.CompilerParams(collective_id=0, has_side_effects=True, vmem_limit_bytes=28 * 1024 * 1024),
        name="gather",
    )(
        *(
            pltpu.with_memory_space_constraint(operand, pltpu.HBM)
            for operand in (weight_up, low_up.T, high_up, norm_train.reshape(1, piece), norm_step.reshape(1, piece))
        )
    )
    ready, scale, serve = pl.pallas_call(
        scale_kernel,
        out_shape=(
            jax.ShapeDtypeStruct((depth, inner), jnp.bfloat16),
            jax.ShapeDtypeStruct((1, depth), jnp.float32),
            jax.ShapeDtypeStruct((96, 128), jnp.bfloat16),
        ),
        in_specs=[in_vmem] * 3,
        out_specs=(anywhere,) * 3,
        scratch_shapes=[
            pltpu.VMEM((depth, inner), jnp.bfloat16),
            pltpu.VMEM((1, depth), jnp.float32),
            pltpu.VMEM((96, 128), jnp.bfloat16),
            pltpu.SemaphoreType.DMA((depth // 16 + 2,)),
        ],
        compiler_params=pltpu.CompilerParams(vmem_limit_bytes=28 * 1024 * 1024),
        name="scale",
    )(latest, tops, norm)
    return ready.T, scale.reshape(depth), serve.reshape(96 * 128)


def solution(mesh):
    finer = Mesh(mesh.devices.reshape(NZ, NX, NC, NW), ("z", "x", "c", "w"))
    return jax.shard_map(
        shards,
        mesh=finer,
        in_specs=(P(ZERO, "w"), P(ZERO, None), P(None, "w"), P(ZERO + ("w",)), P(ZERO + ("w",))),
        out_specs=(P(None, ("w",) + ZERO), P(("w",) + ZERO), P()),
        check_vma=False,
    )
```

```python
import jax
import jax.numpy as jnp
from jax import lax
from jax.experimental import pallas as pl
from jax.experimental.pallas import tpu as pltpu
from jax.sharding import Mesh
from jax.sharding import PartitionSpec as P

NZ, NX, NC, NW = 8, 4, 2, 4
CHIPS = NZ * NX
MESH = pl.DeviceIdType.MESH
ZERO = ("z", "x", "c")

MIX_RATE = 2.0
ORDER = (0, 1, 4, 28, 3, 13, 26, 7, 20, 14, 27, 8, 21, 2, 15, 9, 22, 16, 29, 10, 23, 17, 30, 11, 24, 5, 18, 31, 12, 25, 6, 19)
FIRST = 4
MORE = (0, 0, 5, 22, 0, 0)


def gather_kernel(
    weight, low_t, high, train, step,
    latest, tops, norm,
    buf, low_all, norm_all, high_own, high_turned, pick, rows,
    send_sem, block_sem, turn_sem, phase_send, phase_recv, round_sem, local_sem,
):
    z, x, c, w = (lax.axis_index(name) for name in ("z", "x", "c", "w"))
    other = 1 - c
    me = z * NX + x
    depth, rank = weight.shape[0], low_t.shape[0]
    share = rank // NW

    def at(dz=0, dx=0, dw=0, core=c):
        return {
            "z": lax.rem(z + dz + NZ, NZ),
            "x": lax.rem(x + dx + NX, NX),
            "c": core,
            "w": lax.rem(w + dw + NW, NW),
        }

    def shift(k):
        word, place = k // 6, lax.rem(k, 6)
        packed, below = jnp.int32(0), jnp.int32(1)
        for i in range(6):
            packed = jnp.where(word == i, sum(o << 5 * n for n, o in enumerate(ORDER[6 * i : 6 * i + 6])), packed)
            below = jnp.where(place == i, 1 << 5 * i, below)
        o = lax.rem(packed // below, 32)
        return o // NX, lax.rem(o, NX)

    def remote(src, dst, send, recv, where):
        return pltpu.make_async_remote_copy(
            src_ref=src, dst_ref=dst, send_sem=send, recv_sem=recv, device_id=where, device_id_type=MESH
        )

    barrier = pltpu.get_barrier_semaphore()
    near = [(dz, dx, 0, core) for dz in (1, NZ - 1) for dx in range(NX) for core in (c, other)]
    near += [(0, dx, 0, core) for dx in range(1, NX) for core in (c, other)]
    near += [(0, 0, 0, other)] + [(0, 0, dw, c) for dw in range(1, NW)]
    for where in near:
        pl.semaphore_signal(barrier, 1, device_id=at(*where), device_id_type=MESH)
    pl.semaphore_wait(barrier, len(near))

    def tell(r):
        for dz in (1, NZ - 1):
            pl.semaphore_signal(round_sem.at[r], 1, device_id=at(dz), device_id_type=MESH)

    def hear(r):
        pl.semaphore_wait(round_sem.at[r], 2)

    mine = pl.ds(pl.multiple_of(c * depth, 64), depth)
    part = pl.ds(pl.multiple_of(w * share, 16), share)

    def pair(phase, low_from, low_to, norm_from, norm_to, where):
        return [
            remote(low_from, low_to, phase_send.at[phase % 2, 0], phase_recv.at[phase, 0], where),
        ] + [remote(a, b, phase_send.at[phase % 2, 1], phase_recv.at[phase, 1], where) for a, b in zip(norm_from, norm_to)]

    def z_copies(dz):
        here = norm_all.at[c, x, z, w]
        return pair(0, low_t.at[part, :], low_all.at[c, x, z, part, :], (train, step), (here.at[0], here.at[1]), at(dz))

    def x_copies():
        low, gain = low_all.at[c, x, :, part, :], norm_all.at[c, x, :, w]
        return [copy for dx in range(1, NX) for copy in pair(1, low, low, (gain,), (gain,), at(0, dx))]

    def y_copies():
        low, gain = low_all.at[c, :, :, part, :], norm_all.at[c, :, :, w]
        return [copy for dw in range(1, NW) for copy in pair(2, low, low, (gain,), (gain,), at(dw=dw))]

    def core_copies():
        return pair(3, low_all.at[c], low_all.at[c], (norm_all.at[c],), (norm_all.at[c],), at(core=other))

    bytes_of = (
        (low_all.at[0, 0, pl.ds(0, NZ - 1), part, :], norm_all.at[0, 0, pl.ds(0, NZ - 1), 0]),
        (low_all.at[0, pl.ds(0, NX - 1), :, part, :], norm_all.at[0, pl.ds(0, NX - 1), :, 0]),
        (low_all.at[0, :, :, pl.ds(0, share * (NW - 1)), :], norm_all.at[0, :, :, pl.ds(0, NW - 1)]),
        (low_all.at[0], norm_all.at[0]),
    )

    def wait_bytes(of, sem):
        pltpu.make_async_copy(of, of, sem).wait()

    def wait_phase(phase, sems):
        for kind in range(2):
            wait_bytes(bytes_of[phase][kind], sems.at[phase % sems.shape[0], kind])

    def full_copy(k):
        dz, dx = shift(k)
        there = lax.rem(z + dz, NZ) * NX + lax.rem(x + dx, NX)
        columns = pl.ds(pl.multiple_of(there * 384 + c * 128, 128), 256)
        return remote(weight.at[:, columns], buf.at[me, mine, :], send_sem.at[0], block_sem.at[k], at(dz, dx))

    def part_copy(k):
        dz, dx = shift(k)
        there = lax.rem(z + dz, NZ) * NX + lax.rem(x + dx, NX)
        columns = pl.ds(pl.multiple_of(there * 384 + other * 256, 128), 128)
        lanes = pl.ds(pl.multiple_of(other * 128, 128), 128)
        return remote(weight.at[:, columns], buf.at[me, mine, lanes], send_sem.at[1], block_sem.at[k], at(dz, dx, 0, other))

    def source(k):
        dz, dx = shift(k)
        return lax.rem(z - dz + NZ, NZ), lax.rem(x - dx + NX, NX)

    def turn_copy(k):
        sz, sx = source(k)
        from_chip = sz * NX + sx
        return remote(
            buf.at[from_chip, mine, pl.ds(pl.multiple_of(other * 128, 128), 128)],
            buf.at[from_chip, mine, pl.ds(pl.multiple_of(c * 128, 128), 128)],
            send_sem.at[1], turn_sem.at[lax.rem(k, 4)], at(core=other),
        )

    def send(k, carry=0):
        full_copy(k).start()
        part_copy(k).start()
        return carry

    own = [
        pltpu.make_async_copy(weight.at[:, pl.ds(pl.multiple_of(me * 384 + c * 128, 128), 256)], buf.at[me, mine, :], local_sem.at[0]),
        pltpu.make_async_copy(low_t.at[part, :], low_all.at[c, x, z, part, :], local_sem.at[1]),
        pltpu.make_async_copy(high.at[:, pl.ds(pl.multiple_of(me * 384, 128), 384)], high_own, local_sem.at[2]),
        pltpu.make_async_copy(train, norm_all.at[c, x, z, w, 0], local_sem.at[3]),
        pltpu.make_async_copy(step, norm_all.at[c, x, z, w, 1], local_sem.at[4]),
    ]
    sent = 1

    def send_more(count):
        nonlocal sent
        lax.fori_loop(sent, sent + count, send, 0)
        sent += count

    tell(0)
    for dz in (1, NZ - 1):
        for copy in z_copies(dz):
            copy.start()
    send_more(FIRST)
    for copy in own:
        copy.start()
    for r in range(3):
        hear(r)
        if r < 2:
            tell(r + 1)
        for dz in sorted({2 + r, NZ - 2 - r}):
            for copy in z_copies(dz):
                copy.start()
        send_more(MORE[r])
    part_copy(0).start()

    for copy in own:
        copy.wait()
    turn_copy(0).start()
    high_turned[...] = high_own[...].astype(jnp.float32).T
    column = lax.broadcasted_iota(jnp.int32, pick.shape, 1)
    row = lax.broadcasted_iota(jnp.int32, pick.shape, 0)
    pick[...] = jnp.where(column == row + c * 64, 1.0, 0.0).astype(jnp.bfloat16)
    tops[...] = jnp.zeros_like(tops)

    for phase, following in enumerate((x_copies, y_copies, core_copies)):
        wait_phase(phase, phase_recv)
        if phase > 0:
            wait_phase(phase - 1, phase_send)
        for copy in following():
            copy.start()
        send_more(MORE[3 + phase])
    wait_phase(3, phase_recv)
    lead = sent - 1

    for core in range(NC):
        for width in range(NW):
            def piece(chip, carry):
                both = norm_all[core, lax.rem(chip, NX), chip // NX, width]
                rows[core * NW + width, pl.ds(chip, 1), :] = both[0] + both[1]
                return carry
            lax.fori_loop(0, CHIPS, piece, 0)
    size = train.shape[1]
    flat = jnp.zeros((CHIPS, 384), jnp.float32)
    for i in range(NC * NW):
        spread = (
            lax.broadcasted_iota(jnp.int32, (size, 384), 1) == lax.broadcasted_iota(jnp.int32, (size, 384), 0) + i * size
        )
        flat += jnp.dot(
            rows[i].astype(jnp.bfloat16), jnp.where(spread, 1.0, 0.0).astype(jnp.bfloat16), preferred_element_type=jnp.float32
        )
    total = jnp.zeros(norm.shape, jnp.float32)
    for t in range(3):
        spread = lax.broadcasted_iota(jnp.int32, (96, CHIPS), 0) == 3 * lax.broadcasted_iota(jnp.int32, (96, CHIPS), 1) + t
        total += jnp.dot(
            jnp.where(spread, 1.0, 0.0).astype(jnp.bfloat16),
            flat[:, t * 128 : (t + 1) * 128].astype(jnp.bfloat16),
            preferred_element_type=jnp.float32,
        )
    norm[...] = total

    def work(k, row, count, lane):
        sz, sx = source(k)
        chip = sz * NX + sx
        out, lanes = pl.ds(pl.multiple_of(row, 64), count), pl.ds(pl.multiple_of(lane, 128), 128)
        factor = high_turned[pl.ds(pl.multiple_of(c * depth + row, 64), count), :].astype(jnp.bfloat16)
        base = lax.dot_general(pick[out, lanes], buf[chip, :, lanes], (((1,), (1,)), ((), ())), preferred_element_type=jnp.float32)
        change = jnp.concatenate(
            [jnp.dot(factor, low_all[core, sx, sz], preferred_element_type=jnp.float32) for core in range(NC)], axis=1
        )
        value = base + MIX_RATE * change
        latest[out, pl.ds(pl.multiple_of(chip * 384, 128), 384)] = value
        size_of = jnp.abs(value)
        top = jnp.maximum(jnp.maximum(size_of[:, :128], size_of[:, 128:256]), size_of[:, 256:])
        tops[out, :] = jnp.maximum(tops[out, :], top)

    def work_own(k):
        work(k, c * 64, 128, c * 128)

    def work_turned(k):
        turn_copy(k).wait_recv()
        work(k, other * 128, 64, other * 128)

    wait_bytes(buf.at[0, pl.ds(0, depth), pl.ds(0, 128)], block_sem.at[0])
    work_own(0)

    def main(k, carry):
        wait_bytes(buf.at[0, pl.ds(0, depth * 3 // 2), :], block_sem.at[k])
        turn_copy(k).start()

        @pl.when(k + lead < CHIPS)
        def _():
            send(k + lead)

        work_own(k)
        work_turned(k - 1)
        return carry

    lax.fori_loop(1, CHIPS, main, 0)
    work_turned(CHIPS - 1)

    for phase in (2, 3):
        wait_phase(phase, phase_send)
    wait_bytes(buf.at[pl.ds(0, CHIPS - 1), pl.ds(0, depth), :], send_sem.at[0])
    wait_bytes(buf.at[:, pl.ds(0, depth), :], send_sem.at[1])


def scale_kernel(latest, tops, norm, ready, scale, serve, narrow, scale_row, serve_rows, sems):
    top = jnp.max(tops[...], axis=1, keepdims=True)
    inverse = 1.0 / top
    block = 16
    copies = []
    for i in range(latest.shape[0] // block):
        at = pl.ds(i * block, block)
        narrow[at, :] = (latest[at, :] * inverse[i * block : (i + 1) * block]).astype(jnp.bfloat16)
        copies.append(pltpu.make_async_copy(narrow.at[at, :], ready.at[at, :], sems.at[i]))
        copies[-1].start()
        if i == 0:
            scale_row[...] = jnp.max(tops[...].T, axis=0, keepdims=True)
            serve_rows[...] = norm[...].astype(jnp.bfloat16)
            copies.append(pltpu.make_async_copy(scale_row, scale, sems.at[latest.shape[0] // block]))
            copies[-1].start()
            copies.append(pltpu.make_async_copy(serve_rows, serve, sems.at[latest.shape[0] // block + 1]))
            copies[-1].start()
    for copy in copies:
        copy.wait()


def shards(weight_up, low_up, high_up, norm_train, norm_step):
    depth, inner = weight_up.shape
    rank = low_up.shape[1]
    piece = norm_train.shape[0]
    anywhere = pl.BlockSpec(memory_space=pltpu.HBM)
    in_vmem = pl.BlockSpec(memory_space=pltpu.VMEM)
    latest, tops, norm = pl.pallas_call(
        gather_kernel,
        out_shape=(
            jax.ShapeDtypeStruct((depth, inner), jnp.float32),
            jax.ShapeDtypeStruct((depth, 128), jnp.float32),
            jax.ShapeDtypeStruct((96, 128), jnp.float32),
        ),
        in_specs=[anywhere] * 5,
        out_specs=(in_vmem,) * 3,
        scratch_shapes=[
            pltpu.VMEM((CHIPS, 2 * depth, 256), jnp.bfloat16),
            pltpu.VMEM((NC, NX, NZ, rank, depth), jnp.bfloat16),
            pltpu.VMEM((NC, NX, NZ, NW, 2, 1, piece), jnp.float32),
            pltpu.VMEM((rank, 384), jnp.bfloat16),
            pltpu.VMEM((384, rank), jnp.float32),
            pltpu.VMEM((depth, 256), jnp.bfloat16),
            pltpu.VMEM((NC * NW, CHIPS, piece), jnp.float32),
            pltpu.SemaphoreType.DMA((2,)),
            pltpu.SemaphoreType.DMA((CHIPS,)),
            pltpu.SemaphoreType.DMA((4,)),
            pltpu.SemaphoreType.DMA((2, 2)),
            pltpu.SemaphoreType.DMA((4, 2)),
            pltpu.SemaphoreType.REGULAR((3,)),
            pltpu.SemaphoreType.DMA((5,)),
        ],
        compiler_params=pltpu.CompilerParams(collective_id=0, has_side_effects=True, vmem_limit_bytes=28 * 1024 * 1024),
        name="gather",
    )(
        *(
            pltpu.with_memory_space_constraint(operand, pltpu.HBM)
            for operand in (weight_up, low_up.T, high_up, norm_train.reshape(1, piece), norm_step.reshape(1, piece))
        )
    )
    ready, scale, serve = pl.pallas_call(
        scale_kernel,
        out_shape=(
            jax.ShapeDtypeStruct((depth, inner), jnp.bfloat16),
            jax.ShapeDtypeStruct((1, depth), jnp.float32),
            jax.ShapeDtypeStruct((96, 128), jnp.bfloat16),
        ),
        in_specs=[in_vmem] * 3,
        out_specs=(anywhere,) * 3,
        scratch_shapes=[
            pltpu.VMEM((depth, inner), jnp.bfloat16),
            pltpu.VMEM((1, depth), jnp.float32),
            pltpu.VMEM((96, 128), jnp.bfloat16),
            pltpu.SemaphoreType.DMA((depth // 16 + 2,)),
        ],
        compiler_params=pltpu.CompilerParams(vmem_limit_bytes=28 * 1024 * 1024),
        name="scale",
    )(latest, tops, norm)
    return ready.T, scale.reshape(depth), serve.reshape(96 * 128)


def solution(mesh):
    finer = Mesh(mesh.devices.reshape(NZ, NX, NC, NW), ("z", "x", "c", "w"))
    return jax.shard_map(
        shards,
        mesh=finer,
        in_specs=(P(ZERO, "w"), P(ZERO, None), P(None, "w"), P(ZERO + ("w",)), P(ZERO + ("w",))),
        out_specs=(P(None, ("w",) + ZERO), P(("w",) + ZERO), P()),
        check_vma=False,
    )
```
